256 devices in a mesh: rel: 8 (over x, core), dst: 16 (over z, y_lo), mp: 2 (over y_hi).
Axes of the slice: x: 4, y: 4 (y_hi: 2, y_lo: 2; y = y_hi * 2 + y_lo), z: 8, core: 2. Of those that a mesh axis runs over, the one named last changes fastest.
Arguments:
- node_table: bfloat16 [131072, 512], P(('rel', 'dst')), may hold values from -6 to 6
- edge_weights: bfloat16 [8, 512, 128, 128], P('rel', 'dst'), may hold values from -0.5 to 0.5
- src_ids: int32 [8, 512, 128], P('rel', 'dst'), may hold values from 0 to 1023
- dst_ids: int32 [8, 512, 128], P('rel', 'dst'), may hold values from 0 to 1023
- block_mask: int32 [8, 512], P('rel', 'dst'), may hold values 0 or 1
- basis_coef: float32 [8, 32], P('rel'), may hold values from -0.1875 to 0.1875
- basis_mats: bfloat16 [32, 512, 512], P(None, None, 'mp'), may hold values from -0.25 to 0.25
- type_bias: float32 [4, 512], P(None, 'mp'), may hold values from -3 to 3
- type_rows: int32 [4], replicated, may hold values from 1 to 512, 1024 in all
- cotangent: bfloat16 [16384, 512], P(('rel', 'dst'), 'mp'), may hold values from -0.0014648438 to 0.0014648438
Outputs:
- layer_out: bfloat16 [16384, 512], P(('rel', 'dst'), 'mp')
- coef_grad: float32 [8, 32], P('rel')
The draws below stay inside these ranges and needn't reach their ends.
Inputs may be any that keep to these rules, and one draw needn't show every extreme that they name: `type_rows`: the 4 counts sum to 1024.
All inputs are finite; a program needn't handle non-finite values. No bound on the sum of `block_mask` on one device may be relied on, other than what follows from the above.
Results may differ from the reference program's by a relative error of at most 0.0062.
Values may be sent and summed in bfloat16 or wider, within the bound.
A program may use at most 64 MiB of HBM per device.

```python
import math
import jax
import jax.numpy as jnp
import numpy as np
from jax import lax

F = 512
BASES = 32
BLK = 128
TYPES = 4
BPO = 2
ROWS_DEV = 128
TAB_DEV = 1024
RELATIONS = 8
NBLK = 32
OWN = 1024
TABLE = 131072
OUTROWS = 16384
N_REL = 8
N_DST = 16


def plant(result, stream_key, least, high):
    place = [jax.random.randint(jax.random.fold_in(stream_key, axis), (), 0, length) for axis, length in enumerate(result.shape)]
    widest = result.shape.index(max(result.shape))
    neighbour = place[:widest] + [(place[widest] + 1) % result.shape[widest]] + place[widest + 1:]
    return result.at[tuple(place)].set(least).at[tuple(neighbour)].set(high)


def shard_levels(rng, extent, cuts, smallest, largest):
    level, own = 1.0, jax.random.fold_in(rng, 6)
    for dim, parts in cuts:
        steps = jnp.exp(jax.random.uniform(jax.random.fold_in(own, dim), (parts,), jnp.float32, smallest / len(cuts), largest / len(cuts)))
        level = level * jnp.repeat(steps, extent[dim] // parts).reshape([-1 if axis == dim else 1 for axis in range(len(extent))])
    return level


def split_up(amount, total, most, lean):
    loads = [(1 << 20) // math.isqrt(grade ** lean) + 1 for grade in range(2, amount + 1)]
    spare, holding = total - most - (amount - 1), [1] * (amount - 1)
    while spare > 0:
        free = [i for i in range(amount - 1) if holding[i] < most]
        whole, budget = sum([loads[i] for i in free]), spare
        for i in free:
            extra = min(most - holding[i], max(1, budget * loads[i] // whole), spare)
            holding[i] = holding[i] + extra
            spare = spare - extra
    return np.array([most] + holding)


def ragged(stream_key, number_of, total, limit, lean):
    if number_of == 2:
        one = jax.random.randint(stream_key, (), max(1, total - limit), min(limit, total - 1) + 1)
        return jnp.stack([one, total - one])
    sizes = jnp.asarray(split_up(number_of, total, limit, lean), jnp.int32)
    couples = (number_of - 1) // 2
    giver, receiver = sizes[1:1 + 2 * couples:2], sizes[2:2 + 2 * couples:2]
    margin = jnp.minimum(giver - 1, limit - receiver)
    moved = jax.random.randint(jax.random.fold_in(stream_key, 1), (couples,), 0, 1 << 20) % (margin + 1)
    sizes = sizes.at[1:1 + 2 * couples:2].set(giver - moved).at[2:2 + 2 * couples:2].set(receiver + moved)
    return sizes[jax.random.permutation(jax.random.fold_in(stream_key, 2), number_of)]


def scatter_about(own_key, shape, spread, most, cuts=(), kind=jnp.bfloat16):
    drawn = spread * jax.random.normal(own_key, shape, jnp.float32)
    if cuts:
        drawn = drawn * shard_levels(own_key, shape, cuts, -0.22, 0.18)
    return jnp.clip(drawn, -most, most).astype(kind)


def setup_inputs(seed: int = 0) -> dict:
    splits = jax.random.split(jax.random.key(seed), 11)
    return {
        "node_table": scatter_about(splits[0], (TABLE, F), 1.0, 6.0, ((0, 128),)),
        "edge_weights": scatter_about(splits[1], (RELATIONS, N_DST * NBLK, BLK, BLK), BLK ** -0.5, 0.5, ((0, 8), (1, 16))),
        "src_ids": plant(jax.random.randint(splits[2], (RELATIONS, N_DST * NBLK, BLK), 0, TAB_DEV), jax.random.fold_in(splits[2], 1), 0, TAB_DEV - 1).astype(jnp.int32),
        "dst_ids": plant(jax.random.randint(splits[3], (RELATIONS, N_DST * NBLK, BLK), 0, OWN), jax.random.fold_in(splits[3], 1), 0, OWN - 1).astype(jnp.int32),
        "block_mask": plant((jax.random.randint(splits[4], (RELATIONS, N_DST * NBLK), 0, 3) < 2).astype(jnp.int32), jax.random.fold_in(splits[4], 1), 0, 1),
        "basis_coef": scatter_about(splits[5], (RELATIONS, BASES), (BASES * NBLK * BLK // ROWS_DEV) ** -0.5, 0.1875, ((0, 8),), jnp.float32),
        "basis_mats": scatter_about(splits[6], (BASES, F, F), F ** -0.5, 0.25, ((2, 2),)),
        "type_bias": scatter_about(splits[7], (TYPES, F), 0.5, 3.0, ((1, 2),), jnp.float32),
        "type_rows": ragged(splits[8], TYPES, OWN, OWN // 2, 2).astype(jnp.int32),
        "cotangent": scatter_about(splits[9], (OUTROWS, F), (N_DST * NBLK * BLK * F // 2) ** -0.5, 0.0014648438, ((0, 128), (1, 2))),
    }


highest = lax.Precision.HIGHEST


def reference(node_table, edge_weights, src_ids, dst_ids, block_mask, basis_coef, basis_mats, type_bias, type_rows, cotangent):
    features = node_table.shape[1]
    owner_span = ROWS_DEV * N_REL
    basis_full = basis_mats.astype(jnp.float32)
    mixing = jnp.einsum('rb,bfg->rfg', basis_coef, basis_full, precision=highest).astype(jnp.bfloat16)
    owner_grad = cotangent.reshape(N_REL, N_DST, ROWS_DEV, features).transpose(1, 0, 2, 3).reshape(N_DST, owner_span, features)
    owners = jnp.arange(NBLK, dtype=jnp.int32) // BPO
    owner_rows = jnp.broadcast_to(owners[:, None], (NBLK, BLK)).reshape(-1)

    def visit(state_pair, pair_index):
        summed, basis_grads = state_pair
        relation = pair_index // N_DST
        source = pair_index % N_DST
        zero = jnp.zeros((), jnp.int32)
        table_rows = lax.dynamic_slice_in_dim(node_table, ((relation * N_DST + source) * TAB_DEV).astype(jnp.int32), TAB_DEV, 0)
        start = (source * NBLK).astype(jnp.int32)
        source_ids = lax.dynamic_slice(src_ids, (relation, start, zero), (1, NBLK, BLK))[0]
        slot_ids = lax.dynamic_slice(dst_ids, (relation, start, zero), (1, NBLK, BLK))[0].reshape(-1)
        blocks = lax.dynamic_slice(edge_weights, (relation, start, zero, zero), (1, NBLK, BLK, BLK))[0].astype(jnp.float32)
        live_blocks = lax.dynamic_slice(block_mask, (relation, start), (1, NBLK))[0].astype(jnp.float32)
        picked = table_rows[source_ids.reshape(-1)].reshape(NBLK, BLK, features).astype(jnp.float32)
        messages = jnp.einsum('kij,kjf->kif', blocks * live_blocks[:, None, None], picked, precision=highest)
        messages = messages.astype(jnp.bfloat16).reshape(-1, features).astype(jnp.float32)
        weight = mixing[relation].astype(jnp.float32)
        outgoing = jnp.dot(messages, weight, precision=highest).astype(jnp.bfloat16)
        summed = summed.at[owner_rows, slot_ids].add(outgoing.astype(jnp.float32))
        wanted = owner_grad[owner_rows, slot_ids].astype(jnp.float32)
        outer_sum = jnp.dot(messages.T, wanted, precision=highest)
        update = jnp.einsum('bfg,fg->b', basis_full, outer_sum, precision=highest)
        basis_grads = basis_grads.at[relation].add(update)
        return (summed, basis_grads), None

    start_state = (jnp.zeros((N_DST, owner_span, features), jnp.float32), jnp.zeros((N_REL, BASES), jnp.float32))
    (summed, basis_grads), _ = lax.scan(visit, start_state, jnp.arange(N_REL * N_DST, dtype=jnp.int32))
    bounds = jnp.cumsum(type_rows)
    position = jnp.arange(owner_span, dtype=jnp.int32)
    row_kind = jnp.minimum(jnp.sum((position[:, None] >= bounds[None, :]).astype(jnp.int32), axis=1), TYPES - 1)
    row_bias = type_bias[row_kind]
    layer_out = (summed + row_bias[None]).reshape(N_DST, N_REL, ROWS_DEV, features).transpose(1, 0, 2, 3)
    layer_out = layer_out.reshape(-1, features).astype(jnp.bfloat16)
    return layer_out, basis_grads
```

```python
import jax
import jax.numpy as jnp
from jax import lax
from jax.experimental import pallas as pl
from jax.experimental.pallas import tpu as pltpu
from jax.sharding import PartitionSpec as P

MESH = pl.DeviceIdType.MESH
BF = jnp.bfloat16
F32 = jnp.float32
NX, NC, NZ, NY, NM = 4, 2, 8, 2, 2
NR, ND = NX * NC, NZ * NY
TAB, F, H, BLK, ROWS, BASES = 1024, 512, 256, 128, 128, 32
OWN = NR * ROWS
CHUNK = 2 * BLK


def offset(k):
    step = k // 2
    far = (step // 2 + 1) * (1 - 2 * (step % 2)) * (1 - step // (NZ - 1))
    return far, k % 2


def kernel(
    table, edge, src_ids, dst_ids, mask, coef, basis, bias, type_rows, cot,
    out, grad,
    tbl, edg, sid, bas, hot, sbuf, rbuf, ids, hot_t, acc, accb, gbuf, wall, wbuf,
    s_send, s_recv, s_all, z_sib, z_sibr, z_own, z_send, z_recv, part, p_send, p_recv,
    load_sem, c_ss, c_rs, i_ss, i_rs, g_ss, g_rs, w_sem, s_sem, sib_sem, z_ss, z_rs, p_ss, p_rs,
):
    rel, dst, mp = lax.axis_index("rel"), lax.axis_index("dst"), lax.axis_index("mp")
    x, core = rel // NC, rel % NC
    z, y = dst // NY, dst % NY
    other = 1 - mp

    def load(i, src, to):
        return pltpu.make_async_copy(src, to, load_sem.at[i])

    loads = [
        load(0, table.at[:, pl.ds(pl.multiple_of(mp * H, H), H)], tbl),
        load(1, edge, edg),
        load(2, src_ids, sid),
        load(3, cot, gbuf.at[mp, pl.ds(pl.multiple_of(rel * ROWS, ROWS), ROWS)]),
        load(4, dst_ids.at[dst], ids.at[dst]),
        load(5, basis, bas),
    ]
    for copy in loads:
        copy.start()

    barrier = pltpu.get_barrier_semaphore()

    def greet_dst(q, _):
        to = {"dst": (dst + q // NM) % ND, "mp": (mp + q % NM) % NM}
        pl.semaphore_signal(barrier, inc=1, device_id=to, device_id_type=MESH)
        return 0

    def greet_rel(q, _):
        to = {"rel": (rel + q // NM) % NR, "mp": (mp + q % NM) % NM}
        pl.semaphore_signal(barrier, inc=1, device_id=to, device_id_type=MESH)
        return 0

    lax.fori_loop(1, ND * NM, greet_dst, 0)
    lax.fori_loop(NM, NR * NM, greet_rel, 0)

    lanes = lax.broadcasted_iota(jnp.int32, (BLK, BLK), 1)

    def make_chunk(d, to):
        for half in range(2):
            k = 2 * d + half
            row = sid[pl.ds(k, 1), :]
            col = jnp.broadcast_to(row, (BLK, BLK)).T
            for t in range(TAB // BLK):
                hot[half * BLK : (half + 1) * BLK, t * BLK : (t + 1) * BLK] = jnp.where(
                    lanes + t * BLK == col, 1.0, 0.0
                ).astype(BF)
        picked = jnp.dot(hot[...], tbl[...], preferred_element_type=F32).astype(BF)
        for half in range(2):
            k = 2 * d + half
            live = mask[0, k].astype(F32)
            block = (edg[k].astype(F32) * live).astype(BF)
            to[half * BLK : (half + 1) * BLK, :] = jnp.dot(
                block, picked[half * BLK : (half + 1) * BLK, :], preferred_element_type=F32
            ).astype(BF)

    for i in (0, 1, 2):
        loads[i].wait()
    make_chunk(dst, rbuf.at[dst])
    loads[3].wait()
    loads[4].wait()
    pl.semaphore_wait(barrier, ND * NM - 1 + NR * NM - NM)

    def peer(k, sign):
        dz, dy = offset(k)
        return ((z + sign * dz + NZ) % NZ) * NY + (y + dy) % NY

    def kth(i):
        return i + i // (ND - 2)

    def id_copy(k):
        to = peer(k, 1)
        return pltpu.make_async_remote_copy(
            dst_ids.at[to], ids.at[dst], i_ss.at[to], i_rs.at[dst],
            device_id={"dst": to}, device_id_type=MESH)

    def chunk_copy(k):
        to = peer(k, 1)
        return pltpu.make_async_remote_copy(
            sbuf.at[to], rbuf.at[dst], c_ss.at[to], c_rs.at[dst],
            device_id={"dst": to}, device_id_type=MESH)

    def grad_copy(q):
        to_r, to_m = (rel + q // NM) % NR, (mp + q % NM) % NM
        mine = gbuf.at[mp, pl.ds(pl.multiple_of(rel * ROWS, ROWS), ROWS)]
        slot = rel * NM + mp
        return pltpu.make_async_remote_copy(
            mine, mine, g_ss.at[to_r * NM + to_m], g_rs.at[slot],
            device_id={"rel": to_r, "mp": to_m}, device_id_type=MESH)

    def send_ids(i, _):
        id_copy(kth(i)).start()
        return 0

    lax.fori_loop(0, ND - 1, send_ids, 0)

    def send_chunk(i, _):
        k = kth(i)
        to = peer(k, 1)
        make_chunk(to, sbuf.at[to])
        chunk_copy(k).start()
        return 0

    lax.fori_loop(0, ND - 1, send_chunk, 0)

    def send_grad(q, _):
        grad_copy(q).start()
        return 0

    lax.fori_loop(1, NR * NM, send_grad, 0)

    loads[5].wait()
    TILE = 32

    def mix(t, _):
        at = pl.multiple_of(t * TILE, TILE)
        total = coef[0, 0] * bas[0, pl.ds(at, TILE), :].astype(F32)
        for b in range(1, BASES):
            total = total + coef[0, b] * bas[b, pl.ds(at, TILE), :].astype(F32)
        wall[pl.ds(at, TILE), :] = total.astype(BF)
        return 0

    lax.fori_loop(0, F // TILE, mix, 0)
    w_copy = pltpu.make_async_remote_copy(
        wall.at[pl.ds(pl.multiple_of(other * H, H), H)], wbuf.at[mp], w_sem.at[0], w_sem.at[1],
        device_id={"mp": other}, device_id_type=MESH)
    w_copy.start()
    wbuf[mp] = wall[pl.ds(pl.multiple_of(mp * H, H), H), :]

    rows = lax.broadcasted_iota(jnp.int32, (OWN, BLK), 0)

    def add_chunk(s):
        for half in range(2):
            row = ids[s, half : half + 1, :]
            hot_t[:, half * BLK : (half + 1) * BLK] = jnp.where(rows == row, 1.0, 0.0).astype(BF)
        acc[...] += jnp.dot(hot_t[...], rbuf[s], preferred_element_type=F32)

    acc[...] = jnp.zeros_like(acc)
    add_chunk(dst)

    def take_chunk(i, _):
        s = peer(kth(i), -1)
        pltpu.make_async_remote_copy(
            dst_ids.at[s], ids.at[s], i_ss.at[s], i_rs.at[s],
            device_id={"dst": s}, device_id_type=MESH).wait_recv()
        pltpu.make_async_remote_copy(
            sbuf.at[s], rbuf.at[s], c_ss.at[s], c_rs.at[s],
            device_id={"dst": s}, device_id_type=MESH).wait_recv()
        add_chunk(s)
        return 0

    lax.fori_loop(0, ND - 1, take_chunk, 0)

    def take_grad(q, _):
        fr, fm = (rel + q // NM) % NR, (mp + q % NM) % NM
        theirs = gbuf.at[fm, pl.ds(pl.multiple_of(fr * ROWS, ROWS), ROWS)]
        slot = fr * NM + fm
        pltpu.make_async_remote_copy(
            theirs, theirs, g_ss.at[slot], g_rs.at[slot],
            device_id={"rel": fr, "mp": fm}, device_id_type=MESH).wait_recv()
        return 0

    lax.fori_loop(1, NR * NM, take_grad, 0)
    w_copy.wait_recv()

    accb[...] = acc[...].astype(BF)
    contract = (((0,), (0,)), ((), ()))

    def outer(g):
        return lax.dot_general(accb[...], gbuf[g], contract, preferred_element_type=F32)

    s_send[...] = outer(other).astype(BF)
    s_copy = pltpu.make_async_remote_copy(
        s_send, s_recv, s_sem.at[0], s_sem.at[1], device_id={"mp": other}, device_id_type=MESH)
    s_copy.start()

    def times_w(at, g):
        return jnp.dot(accb[pl.ds(pl.multiple_of(at, ROWS), ROWS), :], wbuf[g], preferred_element_type=F32)

    for xx in range(NX):
        for g in range(NM):
            z_sib[xx, g] = times_w((xx * NC + 1 - core) * ROWS, g).astype(BF)
    sib_copy = pltpu.make_async_remote_copy(
        z_sib, z_sibr, sib_sem.at[0], sib_sem.at[1],
        device_id={"rel": x * NC + 1 - core}, device_id_type=MESH)
    sib_copy.start()
    for xx in range(NX):
        for g in range(NM):
            z_own[xx, g] = times_w((xx * NC + core) * ROWS, g)
    s_all[pl.ds(pl.multiple_of(mp * H, H), H), :] = outer(mp)

    sib_copy.wait_recv()

    def z_copy(q):
        tx, tm = (x + q // NM) % NX, (mp + q % NM) % NM
        return pltpu.make_async_remote_copy(
            z_send.at[tx, tm], z_recv.at[x * NM + mp], z_ss.at[tx * NM + tm], z_rs.at[x * NM + mp],
            device_id={"rel": tx * NC + core, "mp": tm}, device_id_type=MESH)

    for q in range(1, NX * NM):
        tx, tm = (x + q // NM) % NX, (mp + q % NM) % NM
        z_send[tx, tm] = (z_own[tx, tm] + z_sibr[tx, tm].astype(F32)).astype(BF)
        z_copy(q).start()
    z_recv[x * NM + mp] = (z_own[x, mp] + z_sibr[x, mp].astype(F32)).astype(BF)

    DT = 16

    def against(base):
        def step(t, sums):
            at = pl.multiple_of(base + t * DT, DT)
            s = s_all[pl.ds(at, DT), :]
            new = []
            for b in range(BASES):
                v = bas[b, pl.ds(at, DT), :].astype(F32) * s
                v = (v[0:8, 0:128] + v[8:16, 0:128]) + (v[0:8, 128:256] + v[8:16, 128:256])
                new.append(sums[b] + v)
            return tuple(new)
        return step

    zeros = tuple(jnp.zeros((8, 128), F32) for _ in range(BASES))
    sums = lax.fori_loop(0, H // DT, against(mp * H), zeros)
    s_copy.wait_recv()
    s_all[pl.ds(pl.multiple_of(other * H, H), H), :] = s_recv[...].astype(F32)
    sums = lax.fori_loop(0, H // DT, against(other * H), sums)
    for b in range(BASES):
        part[b : b + 1, :] = jnp.sum(sums[b], axis=0, keepdims=True)
    mine = jnp.sum(part[...].T, axis=0, keepdims=True)
    me = dst * NM + mp
    p_send[...] = mine
    p_recv[me] = mine

    def part_copy(q):
        td, tm = (dst + q // NM) % ND, (mp + q % NM) % NM
        return pltpu.make_async_remote_copy(
            p_send, p_recv.at[me], p_ss.at[td * NM + tm], p_rs.at[me],
            device_id={"dst": td, "mp": tm}, device_id_type=MESH)

    def send_part(q, _):
        part_copy(q).start()
        return 0

    lax.fori_loop(1, ND * NM, send_part, 0)

    for q in range(1, NX * NM):
        fx, fm = (x + q // NM) % NX, (mp + q % NM) % NM
        slot = fx * NM + fm
        pltpu.make_async_remote_copy(
            z_send.at[fx, fm], z_recv.at[slot], z_ss.at[slot], z_rs.at[slot],
            device_id={"rel": fx * NC + core, "mp": fm}, device_id_type=MESH).wait_recv()
    total = z_recv[0].astype(F32)
    for q in range(1, NX * NM):
        total = total + z_recv[q].astype(F32)
    at = lax.broadcasted_iota(jnp.int32, (ROWS, H), 0) + rel * ROWS
    bound = type_rows[0]
    row_bias = jnp.broadcast_to(bias[0:1, :], (ROWS, H))
    for c in range(1, 4):
        row_bias = jnp.where(at >= bound, bias[c : c + 1, :], row_bias)
        bound = bound + type_rows[c]
    out[...] = (total + row_bias).astype(BF)

    def take_part(q, _):
        fd, fm = (dst + q // NM) % ND, (mp + q % NM) % NM
        slot = fd * NM + fm
        pltpu.make_async_remote_copy(
            p_send, p_recv.at[slot], p_ss.at[slot], p_rs.at[slot],
            device_id={"dst": fd, "mp": fm}, device_id_type=MESH).wait_recv()
        return 0

    lax.fori_loop(1, ND * NM, take_part, 0)
    total = p_recv[0]
    for q in range(1, ND * NM):
        total = total + p_recv[q]
    grad[...] = total

    def done_ids(i, _):
        id_copy(kth(i)).wait_send()
        chunk_copy(kth(i)).wait_send()
        return 0

    def done_grad(q, _):
        grad_copy(q).wait_send()
        return 0

    def done_part(q, _):
        part_copy(q).wait_send()
        return 0

    lax.fori_loop(0, ND - 1, done_ids, 0)
    lax.fori_loop(1, NR * NM, done_grad, 0)
    lax.fori_loop(1, ND * NM, done_part, 0)
    w_copy.wait_send()
    s_copy.wait_send()
    sib_copy.wait_send()
    for q in range(1, NX * NM):
        z_copy(q).wait_send()


def on_device(
    node_table, edge_weights, src_ids, dst_ids, block_mask,
    basis_coef, basis_mats, type_bias, type_rows, cotangent,
):
    anywhere = pl.BlockSpec(memory_space=pl.ANY)
    vmem = pl.BlockSpec(memory_space=pltpu.VMEM)
    smem = pl.BlockSpec(memory_space=pltpu.SMEM)
    dma = pltpu.SemaphoreType.DMA
    return pl.pallas_call(
        kernel,
        out_shape=(
            jax.ShapeDtypeStruct((ROWS, H), BF),
            jax.ShapeDtypeStruct((1, BASES), F32),
        ),
        in_specs=[anywhere, anywhere, anywhere, anywhere, smem, smem, anywhere, vmem, smem, anywhere],
        out_specs=(vmem, vmem),
        scratch_shapes=[
            pltpu.VMEM((TAB, H), BF),
            pltpu.VMEM((2 * ND, BLK, BLK), BF),
            pltpu.VMEM((2 * ND, BLK), jnp.int32),
            pltpu.VMEM((BASES, F, H), BF),
            pltpu.VMEM((CHUNK, TAB), BF),
            pltpu.VMEM((ND, CHUNK, H), BF),
            pltpu.VMEM((ND, CHUNK, H), BF),
            pltpu.VMEM((ND, 2, BLK), jnp.int32),
            pltpu.VMEM((OWN, CHUNK), BF),
            pltpu.VMEM((OWN, H), F32),
            pltpu.VMEM((OWN, H), BF),
            pltpu.VMEM((NM, OWN, H), BF),
            pltpu.VMEM((F, H), BF),
            pltpu.VMEM((NM, H, H), BF),
            pltpu.VMEM((H, H), BF),
            pltpu.VMEM((H, H), BF),
            pltpu.VMEM((F, H), F32),
            pltpu.VMEM((NX, NM, ROWS, H), BF),
            pltpu.VMEM((NX, NM, ROWS, H), BF),
            pltpu.VMEM((NX, NM, ROWS, H), F32),
            pltpu.VMEM((NX, NM, ROWS, H), BF),
            pltpu.VMEM((NX * NM, ROWS, H), BF),
            pltpu.VMEM((BASES, 128), F32),
            pltpu.VMEM((1, BASES), F32),
            pltpu.VMEM((ND * NM, 1, BASES), F32),
            dma((6,)),
            dma((ND,)), dma((ND,)), dma((ND,)), dma((ND,)),
            dma((NR * NM,)), dma((NR * NM,)),
            dma((2,)), dma((2,)), dma((2,)),
            dma((NX * NM,)), dma((NX * NM,)),
            dma((ND * NM,)), dma((ND * NM,)),
        ],
        compiler_params=pltpu.CompilerParams(
            collective_id=0, has_side_effects=True, vmem_limit_bytes=50 * 1024 * 1024
        ),
        name="relational_layer",
    )(
        node_table, edge_weights[0], src_ids[0], dst_ids[0].reshape(ND, 2, BLK), block_mask,
        basis_coef, basis_mats, type_bias, type_rows, cotangent,
    )


def solution(mesh):
    in_specs = (
        P(("rel", "dst"), None),
        P("rel", "dst", None, None),
        P("rel", "dst", None),
        P("rel", "dst", None),
        P("rel", "dst"),
        P("rel", None),
        P(None, None, "mp"),
        P(None, "mp"),
        P(),
        P(("rel", "dst"), "mp"),
    )
    out_specs = (P(("rel", "dst"), "mp"), P("rel", None))
    return jax.shard_map(
        on_device, mesh=mesh, in_specs=in_specs, out_specs=out_specs, check_vma=False
    )
```

```python
import jax
import jax.numpy as jnp
from jax import lax
from jax.experimental import pallas as pl
from jax.experimental.pallas import tpu as pltpu
from jax.sharding import PartitionSpec as P

MESH = pl.DeviceIdType.MESH
BF = jnp.bfloat16
F32 = jnp.float32
NX, NC, NZ, NY, NM = 4, 2, 8, 2, 2
NR, ND = NX * NC, NZ * NY
TAB, F, H, BLK, ROWS, BASES = 1024, 512, 256, 128, 128, 32
OWN = NR * ROWS
CHUNK = 2 * BLK
EARLY = 6


def offset(k):
    step = k // 2
    far = (step // 2 + 1) * (1 - 2 * (step % 2)) * (1 - step // (NZ - 1))
    return far, k % 2


def kernel(
    table, edge, src_ids, dst_ids, mask_any, coef_any, basis, bias_any, rows_any, cot,
    out, grad,
    mask, coef, type_rows, bias,
    tbl, edg, sid, bas, hot, sbuf, rbuf, ids, hot_t, acc, accb, acct, gbuf, wall, wbuf,
    s_send, s_recv, s_all, z_sib, z_sibr, z_own, z_send, z_recv, part, p_send, p_recv,
    load_sem, c_ss, c_rs, i_ss, i_rs, g_ss, g_rs, w_sem, s_sem, sib_ss, sib_rs, z_ss, z_rs, p_ss, p_rs,
):
    rel, dst, mp = lax.axis_index("rel"), lax.axis_index("dst"), lax.axis_index("mp")
    x, core = rel // NC, rel % NC
    z, y = dst // NY, dst % NY
    other = 1 - mp

    def load(i, src, to):
        return pltpu.make_async_copy(src, to, load_sem.at[i])

    def remote(src, to, ss, rs, **where):
        return pltpu.make_async_remote_copy(src, to, ss, rs, device_id=where, device_id_type=MESH)

    loads = [
        load(0, src_ids, sid),
        load(1, mask_any, mask),
        load(2, table.at[:, pl.ds(pl.multiple_of(mp * H, H), H)], tbl),
        load(3, edge, edg),
        load(4, dst_ids.at[dst], ids.at[dst]),
        load(5, cot, gbuf.at[core, mp, x]),
        load(6, coef_any, coef),
        load(7, rows_any, type_rows),
        load(8, bias_any, bias),
        load(9, basis, bas),
    ]
    for copy in loads[:9]:
        copy.start()

    barrier = pltpu.get_barrier_semaphore()
    group = [q for q in range(1, ND * NM)]
    across = [(dx, dm) for dx in range(1, NX) for dm in range(NM)]

    def greet(**where):
        pl.semaphore_signal(barrier, inc=1, device_id=where, device_id_type=MESH)

    for q in group:
        greet(dst=(dst + q // NM) % ND, mp=(mp + q % NM) % NM)
    for dx, dm in across:
        greet(rel=(x + dx) % NX * NC + core, mp=(mp + dm) % NM)
    sibling = x * NC + 1 - core
    greet(rel=sibling)

    lanes = lax.broadcasted_iota(jnp.int32, (BLK, BLK), 1)

    def make_chunk(d, to):
        for half in range(2):
            k = 2 * d + half
            row = sid[pl.ds(k, 1), :]
            col = jnp.broadcast_to(row, (BLK, BLK)).T
            for t in range(TAB // BLK):
                hot[half * BLK : (half + 1) * BLK, t * BLK : (t + 1) * BLK] = jnp.where(
                    lanes + t * BLK == col, 1.0, 0.0
                ).astype(BF)
        picked = jnp.dot(hot[...], tbl[...], preferred_element_type=F32).astype(BF)
        for half in range(2):
            k = 2 * d + half
            live = mask[0, k].astype(F32)
            block = (edg[k].astype(F32) * live).astype(BF)
            to[half * BLK : (half + 1) * BLK, :] = jnp.dot(
                block, picked[half * BLK : (half + 1) * BLK, :], preferred_element_type=F32
            ).astype(BF)

    def peer(k, sign):
        dz, dy = offset(k)
        return ((z + sign * dz + NZ) % NZ) * NY + (y + dy) % NY

    def kth(i):
        return i + i // (ND - 2)

    def id_copy(to):
        return remote(dst_ids.at[to], ids.at[dst], i_ss.at[to], i_rs.at[dst], dst=to)

    def chunk_copy(to):
        return remote(sbuf.at[to], rbuf.at[dst], c_ss.at[to], c_rs.at[dst], dst=to)

    def make(i, _):
        to = peer(kth(i), 1)
        make_chunk(to, sbuf.at[to])
        return 0

    def send(i, _):
        chunk_copy(peer(kth(i), 1)).start()
        return 0

    def send_ids(i, _):
        id_copy(peer(kth(i), 1)).start()
        return 0

    def make_send(i, _):
        make(i, 0)
        return send(i, 0)

    for i in range(4):
        loads[i].wait()
    lax.fori_loop(0, EARLY, make, 0)
    loads[4].wait()
    loads[5].wait()
    pl.semaphore_wait(barrier, len(group) + len(across) + 1)
    lax.fori_loop(0, EARLY, send, 0)
    lax.fori_loop(0, ND - 1, send_ids, 0)
    mine = gbuf.at[core, mp, x]
    g_pair = remote(mine, mine, g_ss.at[0], g_rs.at[0], mp=other)
    g_pair.start()
    loads[9].start()
    lax.fori_loop(EARLY, ND - 1, make_send, 0)
    make_chunk(dst, rbuf.at[dst])

    g_pair.wait_recv()

    def g_across(dx):
        both = gbuf.at[core, :, x]
        return remote(both, both, g_ss.at[dx], g_rs.at[dx], rel=(x + dx) % NX * NC + core)

    for dx in range(1, NX):
        g_across(dx).start()

    for i in (6, 7, 8, 9):
        loads[i].wait()
    TILE = 32

    def mix(t, _):
        at = pl.multiple_of(t * TILE, TILE)
        total = coef[0, 0] * bas[0, pl.ds(at, TILE), :].astype(F32)
        for b in range(1, BASES):
            total = total + coef[0, b] * bas[b, pl.ds(at, TILE), :].astype(F32)
        wall[pl.ds(at, TILE), :] = total.astype(BF)
        return 0

    lax.fori_loop(0, F // TILE, mix, 0)
    w_copy = remote(wall.at[pl.ds(pl.multiple_of(other * H, H), H)], wbuf.at[mp], w_sem.at[0], w_sem.at[1], mp=other)
    w_copy.start()
    wbuf[mp] = wall[pl.ds(pl.multiple_of(mp * H, H), H), :]

    place = lax.broadcasted_iota(jnp.int32, (OWN, BLK), 0)
    half_rows = NX * ROWS
    rows = ((place % half_rows) // ROWS * NC + place // half_rows) * ROWS + place % ROWS

    def add_chunk(s):
        for half in range(2):
            row = ids[s, half : half + 1, :]
            hot_t[:, half * BLK : (half + 1) * BLK] = jnp.where(rows == row, 1.0, 0.0).astype(BF)
        return jnp.dot(hot_t[...], rbuf[s], preferred_element_type=F32)

    acc[...] = add_chunk(dst)

    def take(i):
        s = peer(kth(i), -1)
        remote(dst_ids.at[s], ids.at[s], i_ss.at[s], i_rs.at[s], dst=s).wait_recv()
        remote(sbuf.at[s], rbuf.at[s], c_ss.at[s], c_rs.at[s], dst=s).wait_recv()
        return add_chunk(s)

    def take_chunk(i, _):
        acc[...] += take(i)
        return 0

    lax.fori_loop(0, 8, take_chunk, 0)

    for dx in range(1, NX):
        theirs = gbuf.at[core, :, (x - dx + NX) % NX]
        remote(theirs, theirs, g_ss.at[dx], g_rs.at[dx], rel=(x - dx + NX) % NX * NC + core).wait_recv()
    g_sib = remote(gbuf.at[core], gbuf.at[core], g_ss.at[NX], g_rs.at[NX], rel=sibling)
    g_sib.start()

    lax.fori_loop(8, ND - 2, take_chunk, 0)
    g_sib.wait_recv()
    w_copy.wait_recv()

    accb[...] = (acc[...] + take(ND - 2)).astype(BF)
    acct[...] = accb[...].T

    def outer(g):
        return jnp.dot(acct[...], gbuf[:, g].reshape(OWN, H), preferred_element_type=F32)

    s_send[...] = outer(other).astype(BF)
    s_copy = remote(s_send, s_recv, s_sem.at[0], s_sem.at[1], mp=other)
    s_copy.start()

    def times_w(c, g):
        return jnp.dot(
            accb[pl.ds(pl.multiple_of(c * half_rows, half_rows), half_rows), :], wbuf[g],
            preferred_element_type=F32)

    def sib_copy(g):
        return remote(z_sib.at[g], z_sibr.at[g], sib_ss.at[g], sib_rs.at[g], rel=sibling)

    columns = (other, mp)
    for g in columns:
        z_sib[g] = times_w(1 - core, g).astype(BF)
        sib_copy(g).start()
    for g in columns:
        z_own[g] = times_w(core, g)

    def z_copy(dx, dm):
        tx, tm = (x + dx) % NX, (mp + dm) % NM
        return remote(
            z_send.at[tm, tx], z_recv.at[x * NM + mp], z_ss.at[tx * NM + tm], z_rs.at[x * NM + mp],
            rel=tx * NC + core, mp=tm)

    order = (2, 1, 3, 0)
    for dm in (1, 0):
        g = (mp + dm) % NM
        sib_copy(g).wait_recv()
        for dx in order:
            tx = (x + dx) % NX
            at = pl.ds(pl.multiple_of(tx * ROWS, ROWS), ROWS)
            piece = (z_own[g, at, :] + z_sibr[g, at, :].astype(F32)).astype(BF)
            if dx or dm:
                z_send[g, tx] = piece
                z_copy(dx, dm).start()
            else:
                z_recv[x * NM + mp] = piece

    s_all[pl.ds(pl.multiple_of(mp * H, H), H), :] = outer(mp)
    DT = 16

    def against(base):
        def step(t, sums):
            at = pl.multiple_of(base + t * DT, DT)
            s = s_all[pl.ds(at, DT), :]
            new = []
            for b in range(BASES):
                v = bas[b, pl.ds(at, DT), :].astype(F32) * s
                v = (v[0:8, 0:128] + v[8:16, 0:128]) + (v[0:8, 128:256] + v[8:16, 128:256])
                new.append(sums[b] + v)
            return tuple(new)
        return step

    zeros = tuple(jnp.zeros((8, 128), F32) for _ in range(BASES))
    sums = lax.fori_loop(0, H // DT, against(mp * H), zeros)

    def done_chunk(i, _):
        to = peer(kth(i), 1)
        id_copy(to).wait_send()
        chunk_copy(to).wait_send()
        return 0

    lax.fori_loop(0, ND - 1, done_chunk, 0)
    g_pair.wait_send()
    for dx in range(1, NX):
        g_across(dx).wait_send()
    g_sib.wait_send()
    w_copy.wait_send()

    s_copy.wait_recv()
    s_all[pl.ds(pl.multiple_of(other * H, H), H), :] = s_recv[...].astype(F32)
    sums = lax.fori_loop(0, H // DT, against(other * H), sums)
    for b in range(BASES):
        part[b : b + 1, :] = jnp.sum(sums[b], axis=0, keepdims=True)
    total = jnp.sum(part[...].T, axis=0, keepdims=True)
    me = dst * NM + mp
    p_send[...] = total
    p_recv[me] = total

    def part_copy(q):
        td, tm = (dst + q // NM) % ND, (mp + q % NM) % NM
        return remote(p_send, p_recv.at[me], p_ss.at[q], p_rs.at[q], dst=td, mp=tm)

    for q in group:
        part_copy(q).start()

    at = lax.broadcasted_iota(jnp.int32, (ROWS, H), 0) + rel * ROWS
    bound = type_rows[0]
    row_bias = jnp.broadcast_to(bias[0:1, :], (ROWS, H))
    for c in range(1, 4):
        row_bias = jnp.where(at >= bound, bias[c : c + 1, :], row_bias)
        bound = bound + type_rows[c]
    for dx, dm in across + [(0, 1)]:
        fx, fm = (x - dx + NX) % NX, (mp + dm) % NM
        slot = fx * NM + fm
        remote(
            z_send.at[fm, fx], z_recv.at[slot], z_ss.at[slot], z_rs.at[slot],
            rel=fx * NC + core, mp=fm).wait_recv()
    total = z_recv[0].astype(F32)
    for q in range(1, NX * NM):
        total = total + z_recv[q].astype(F32)
    out[...] = (total + row_bias).astype(BF)

    s_copy.wait_send()
    for dm in (1, 0):
        sib_copy((mp + dm) % NM).wait_send()
    for dx, dm in across + [(0, 1)]:
        z_copy(dx, dm).wait_send()
    for q in group:
        fd, fm = (dst - q // NM + ND) % ND, (mp + q % NM) % NM
        remote(p_send, p_recv.at[fd * NM + fm], p_ss.at[q], p_rs.at[q], dst=fd, mp=fm).wait_recv()
    total = p_recv[0]
    for q in range(1, ND * NM):
        total = total + p_recv[q]
    grad[...] = total
    for q in group:
        part_copy(q).wait_send()


def on_device(
    node_table, edge_weights, src_ids, dst_ids, block_mask,
    basis_coef, basis_mats, type_bias, type_rows, cotangent,
):
    anywhere = pl.BlockSpec(memory_space=pl.ANY)
    vmem = pl.BlockSpec(memory_space=pltpu.VMEM)
    dma = pltpu.SemaphoreType.DMA
    return pl.pallas_call(
        kernel,
        out_shape=(
            jax.ShapeDtypeStruct((ROWS, H), BF),
            jax.ShapeDtypeStruct((1, BASES), F32),
        ),
        in_specs=[anywhere] * 10,
        out_specs=(vmem, vmem),
        scratch_shapes=[
            pltpu.SMEM((1, 2 * ND), jnp.int32),
            pltpu.SMEM((1, BASES), F32),
            pltpu.SMEM((4,), jnp.int32),
            pltpu.VMEM((4, H), F32),
            pltpu.VMEM((TAB, H), BF),
            pltpu.VMEM((2 * ND, BLK, BLK), BF),
            pltpu.VMEM((2 * ND, BLK), jnp.int32),
            pltpu.VMEM((BASES, F, H), BF),
            pltpu.VMEM((CHUNK, TAB), BF),
            pltpu.VMEM((ND, CHUNK, H), BF),
            pltpu.VMEM((ND, CHUNK, H), BF),
            pltpu.VMEM((ND, 2, BLK), jnp.int32),
            pltpu.VMEM((OWN, CHUNK), BF),
            pltpu.VMEM((OWN, H), F32),
            pltpu.VMEM((OWN, H), BF),
            pltpu.VMEM((H, OWN), BF),
            pltpu.VMEM((NC, NM, NX, ROWS, H), BF),
            pltpu.VMEM((F, H), BF),
            pltpu.VMEM((NM, H, H), BF),
            pltpu.VMEM((H, H), BF),
            pltpu.VMEM((H, H), BF),
            pltpu.VMEM((F, H), F32),
            pltpu.VMEM((NM, NX * ROWS, H), BF),
            pltpu.VMEM((NM, NX * ROWS, H), BF),
            pltpu.VMEM((NM, NX * ROWS, H), F32),
            pltpu.VMEM((NM, NX, ROWS, H), BF),
            pltpu.VMEM((NX * NM, ROWS, H), BF),
            pltpu.VMEM((BASES, 128), F32),
            pltpu.VMEM((1, BASES), F32),
            pltpu.VMEM((ND * NM, 1, BASES), F32),
            dma((10,)),
            dma((ND,)), dma((ND,)), dma((ND,)), dma((ND,)),
            dma((NX + 1,)), dma((NX + 1,)),
            dma((2,)), dma((2,)), dma((NM,)), dma((NM,)),
            dma((NX * NM,)), dma((NX * NM,)),
            dma((ND * NM,)), dma((ND * NM,)),
        ],
        compiler_params=pltpu.CompilerParams(
            collective_id=0, has_side_effects=True, vmem_limit_bytes=67000000
        ),
        name="relational_layer",
    )(
        node_table, edge_weights[0], src_ids[0], dst_ids[0].reshape(ND, 2, BLK), block_mask,
        basis_coef, basis_mats, type_bias, type_rows, cotangent,
    )


def solution(mesh):
    in_specs = (
        P(("rel", "dst"), None),
        P("rel", "dst", None, None),
        P("rel", "dst", None),
        P("rel", "dst", None),
        P("rel", "dst"),
        P("rel", None),
        P(None, None, "mp"),
        P(None, "mp"),
        P(),
        P(("rel", "dst"), "mp"),
    )
    out_specs = (P(("rel", "dst"), "mp"), P("rel", None))
    return jax.shard_map(
        on_device, mesh=mesh, in_specs=in_specs, out_specs=out_specs, check_vma=False
    )
```

```python
import jax
import jax.numpy as jnp
from jax import lax
from jax.experimental import pallas as pl
from jax.experimental.pallas import tpu as pltpu
from jax.sharding import PartitionSpec as P

MESH = pl.DeviceIdType.MESH
BF = jnp.bfloat16
F32 = jnp.float32
NX, NC, NZ, NY, NM = 4, 2, 8, 2, 2
NR, ND = NX * NC, NZ * NY
TAB, F, H, BLK, ROWS, BASES = 1024, 512, 256, 128, 128, 32
OWN = NR * ROWS
CHUNK = 2 * BLK
NQ, Q = 2, 128
EARLY = 3


def offset(k):
    step = k // 2
    far = (step // 2 + 1) * (1 - 2 * (step % 2)) * (1 - step // (NZ - 1))
    return far, k % 2


def kernel(
    table, edge, src_ids, dst_ids, mask_any, coef_any, basis, bias_any, rows_any, cot,
    out, grad,
    mask, coef, type_rows, bias,
    tbl, edg, sid, bas, hot, sbuf, rbuf, ids, hot_t, acc, accb, acct, gbuf, wall, wbuf,
    s_send, s_recv, s_all, grad_sums, z_sib, z_sibr, z_own, z_send, z_recv, part, p_send, p_recv,
    load_sem, c_ss, c_rs, i_ss, i_rs, g_ss, g_rs, w_sem, s_ss, s_rs, sib_ss, sib_rs, z_ss, z_rs, p_ss, p_rs,
):
    rel, dst, mp = lax.axis_index("rel"), lax.axis_index("dst"), lax.axis_index("mp")
    x, core = rel // NC, rel % NC
    z, y = dst // NY, dst % NY
    other = 1 - mp

    def load(i, src, to):
        return pltpu.make_async_copy(src, to, load_sem.at[i])

    def remote(src, to, ss, rs, **where):
        return pltpu.make_async_remote_copy(src, to, ss, rs, device_id=where, device_id_type=MESH)

    barrier = pltpu.get_barrier_semaphore()
    group = sorted(range(1, ND * NM), key=lambda q: abs(q - ND))
    across = [(dx, dm) for dx in range(1, NX) for dm in range(NM)]

    def greet(**where):
        pl.semaphore_signal(barrier, inc=1, device_id=where, device_id_type=MESH)

    for q in group:
        greet(dst=(dst + q // NM) % ND, mp=(mp + q % NM) % NM)
    for dx, dm in across:
        greet(rel=(x + dx) % NX * NC + core, mp=(mp + dm) % NM)
    sibling = x * NC + 1 - core
    greet(rel=sibling)

    loads = [
        load(0, src_ids, sid),
        load(1, mask_any, mask),
        load(2, table.at[:, pl.ds(pl.multiple_of(mp * H, H), H)], tbl),
        load(3, edge, edg),
        load(4, dst_ids.at[dst], ids.at[dst]),
        load(5, cot, gbuf.at[core, mp, x]),
        load(6, coef_any, coef),
        load(7, rows_any, type_rows),
        load(8, bias_any, bias),
        load(9, basis, bas),
    ]
    for copy in loads[:9]:
        copy.start()

    lanes = lax.broadcasted_iota(jnp.int32, (BLK, BLK), 1)

    def make_chunk(d, to, at):
        for half in range(2):
            k = 2 * d + half
            row = sid[pl.ds(k, 1), :]
            col = jnp.broadcast_to(row, (BLK, BLK)).T
            for t in range(TAB // BLK):
                hot[half * BLK : (half + 1) * BLK, t * BLK : (t + 1) * BLK] = jnp.where(
                    lanes + t * BLK == col, 1.0, 0.0
                ).astype(BF)
        picked = jnp.dot(hot[...], tbl[...], preferred_element_type=F32).astype(BF)
        for half in range(2):
            k = 2 * d + half
            live = mask[0, k].astype(F32)
            block = (edg[k].astype(F32) * live).astype(BF)
            made = jnp.dot(
                block, picked[half * BLK : (half + 1) * BLK, :], preferred_element_type=F32
            ).astype(BF)
            for q in range(NQ):
                to[q, at, half * BLK : (half + 1) * BLK, :] = made[:, q * Q : (q + 1) * Q]

    def peer(k, sign):
        dz, dy = offset(k)
        return ((z + sign * dz + NZ) % NZ) * NY + (y + dy) % NY

    def kth(i):
        return i + i // (ND - 2)

    def id_copy(to):
        return remote(dst_ids.at[to], ids.at[dst], i_ss.at[to], i_rs.at[dst], dst=to)

    def chunk_copy(to, q):
        return remote(sbuf.at[q, to], rbuf.at[q, dst], c_ss.at[q, to], c_rs.at[q, dst], dst=to)

    def make(i, _):
        to = peer(kth(i), 1)
        make_chunk(to, sbuf, to)
        return 0

    def send(q):
        def start(i, _):
            chunk_copy(peer(kth(i), 1), q).start()
            return 0
        return start

    def send_ids(i, _):
        id_copy(peer(kth(i), 1)).start()
        return 0

    def make_send(i, _):
        make(i, 0)
        return send(0)(i, 0)

    for i in range(4):
        loads[i].wait()
    lax.fori_loop(0, EARLY, make, 0)
    loads[4].wait()
    loads[5].wait()
    pl.semaphore_wait(barrier, len(group) + len(across) + 1)
    lax.fori_loop(0, EARLY, send(0), 0)
    lax.fori_loop(0, ND - 1, send_ids, 0)
    mine = gbuf.at[core, mp, x]
    g_pair = remote(mine, mine, g_ss.at[0], g_rs.at[0], mp=other)
    g_pair.start()
    loads[9].start()
    lax.fori_loop(EARLY, ND - 1, make_send, 0)
    lax.fori_loop(0, ND - 1, send(1), 0)
    make_chunk(dst, rbuf, dst)

    g_pair.wait_recv()

    def g_across(dx):
        both = gbuf.at[core, :, x]
        return remote(both, both, g_ss.at[dx], g_rs.at[dx], rel=(x + dx) % NX * NC + core)

    for dx in range(1, NX):
        g_across(dx).start()

    for i in (6, 7, 8, 9):
        loads[i].wait()
    TILE = 32

    def mix(t, _):
        at = pl.multiple_of(t * TILE, TILE)
        total = coef[0, 0] * bas[0, pl.ds(at, TILE), :].astype(F32)
        for b in range(1, BASES):
            total = total + coef[0, b] * bas[b, pl.ds(at, TILE), :].astype(F32)
        wall[pl.ds(at, TILE), :] = total.astype(BF)
        return 0

    lax.fori_loop(0, F // TILE, mix, 0)
    w_copy = remote(wall.at[pl.ds(pl.multiple_of(other * H, H), H)], wbuf.at[mp], w_sem.at[0], w_sem.at[1], mp=other)
    w_copy.start()
    wbuf[mp] = wall[pl.ds(pl.multiple_of(mp * H, H), H), :]

    place = lax.broadcasted_iota(jnp.int32, (OWN, BLK), 0)
    half_rows = NX * ROWS
    rows = ((place % half_rows) // ROWS * NC + place // half_rows) * ROWS + place % ROWS

    def add_chunk(s, q):
        for half in range(2):
            row = ids[s, half : half + 1, :]
            hot_t[:, half * BLK : (half + 1) * BLK] = jnp.where(rows == row, 1.0, 0.0).astype(BF)
        return jnp.dot(hot_t[...], rbuf[q, s], preferred_element_type=F32)

    for q in range(NQ):
        acc[q] = add_chunk(dst, q)

    def take(i, q):
        s = peer(kth(i), -1)
        if q == 0:
            remote(dst_ids.at[s], ids.at[s], i_ss.at[s], i_rs.at[s], dst=s).wait_recv()
        remote(sbuf.at[q, s], rbuf.at[q, s], c_ss.at[q, s], c_rs.at[q, s], dst=s).wait_recv()
        return add_chunk(s, q)

    def take_chunk(q):
        def step(i, _):
            acc[q] += take(i, q)
            return 0
        return step

    def outer(g, q):
        return jnp.dot(acct[q], gbuf[:, g].reshape(OWN, H), preferred_element_type=F32)

    def s_copy(q):
        return remote(s_send.at[q], s_recv.at[q], s_ss.at[q], s_rs.at[q], mp=other)

    def s_rows(m, q):
        return pl.multiple_of(m * H + q * Q, Q)

    def sums_final(q, total):
        half = total.astype(BF)
        accb[:, q * Q : (q + 1) * Q] = half
        acct[q] = half.T
        s_send[q] = outer(other, q).astype(BF)
        s_copy(q).start()

    DT = 16

    def against(m, q):
        base = s_rows(m, q)
        def step(t, sums):
            at = pl.multiple_of(base + t * DT, DT)
            s = s_all[pl.ds(at, DT), :]
            new = []
            for b in range(BASES):
                v = bas[b, pl.ds(at, DT), :].astype(F32) * s
                v = (v[0:8, 0:128] + v[8:16, 0:128]) + (v[0:8, 128:256] + v[8:16, 128:256])
                new.append(sums[b] + v)
            return tuple(new)
        first = tuple(grad_sums[b] for b in range(BASES))
        sums = lax.fori_loop(0, Q // DT, step, first)
        for b in range(BASES):
            grad_sums[b] = sums[b]

    def against_own(q):
        s_all[pl.ds(s_rows(mp, q), Q), :] = outer(mp, q)
        against(mp, q)

    def against_other(q):
        s_copy(q).wait_recv()
        s_all[pl.ds(s_rows(other, q), Q), :] = s_recv[q].astype(F32)
        against(other, q)

    grad_sums[...] = jnp.zeros_like(grad_sums)
    lax.fori_loop(0, 4, take_chunk(0), 0)

    for dx in range(1, NX):
        theirs = gbuf.at[core, :, (x - dx + NX) % NX]
        remote(theirs, theirs, g_ss.at[dx], g_rs.at[dx], rel=(x - dx + NX) % NX * NC + core).wait_recv()
    g_sib = remote(gbuf.at[core], gbuf.at[core], g_ss.at[NX], g_rs.at[NX], rel=sibling)
    g_sib.start()

    lax.fori_loop(4, ND - 1, take_chunk(0), 0)
    g_sib.wait_recv()
    sums_final(0, acc[0])
    lax.fori_loop(0, 2, take_chunk(1), 0)
    against_own(0)
    lax.fori_loop(2, 6, take_chunk(1), 0)
    against_other(0)
    w_copy.wait_recv()
    lax.fori_loop(6, ND - 2, take_chunk(1), 0)
    sums_final(1, acc[1] + take(ND - 2, 1))

    def times_w(c, g):
        return jnp.dot(
            accb[pl.ds(pl.multiple_of(c * half_rows, half_rows), half_rows), :], wbuf[g],
            preferred_element_type=F32)

    def sib_copy(g):
        return remote(z_sib.at[g], z_sibr.at[g], sib_ss.at[g], sib_rs.at[g], rel=sibling)

    columns = (other, mp)
    for g in columns:
        z_sib[g] = times_w(1 - core, g).astype(BF)
        sib_copy(g).start()
    for g in columns:
        z_own[g] = times_w(core, g)

    def z_copy(dx, dm):
        tx, tm = (x + dx) % NX, (mp + dm) % NM
        return remote(
            z_send.at[tm, tx], z_recv.at[x * NM + mp], z_ss.at[tx * NM + tm], z_rs.at[x * NM + mp],
            rel=tx * NC + core, mp=tm)

    order = (2, 1, 3, 0)
    for dm in (1, 0):
        g = (mp + dm) % NM
        sib_copy(g).wait_recv()
        for dx in order:
            tx = (x + dx) % NX
            at = pl.ds(pl.multiple_of(tx * ROWS, ROWS), ROWS)
            piece = (z_own[g, at, :] + z_sibr[g, at, :].astype(F32)).astype(BF)
            if dx or dm:
                z_send[g, tx] = piece
                z_copy(dx, dm).start()
            else:
                z_recv[x * NM + mp] = piece

    against_own(1)

    def done_chunk(i, _):
        to = peer(kth(i), 1)
        id_copy(to).wait_send()
        for q in range(NQ):
            chunk_copy(to, q).wait_send()
        return 0

    lax.fori_loop(0, ND - 1, done_chunk, 0)
    g_pair.wait_send()
    for dx in range(1, NX):
        g_across(dx).wait_send()
    g_sib.wait_send()
    w_copy.wait_send()

    against_other(1)
    for b in range(BASES):
        part[b : b + 1, :] = jnp.sum(grad_sums[b], axis=0, keepdims=True)
    total = jnp.sum(part[...].T, axis=0, keepdims=True)
    me = dst * NM + mp
    p_send[...] = total
    p_recv[me] = total

    def part_copy(q):
        td, tm = (dst + q // NM) % ND, (mp + q % NM) % NM
        return remote(p_send, p_recv.at[me], p_ss.at[q], p_rs.at[q], dst=td, mp=tm)

    for q in group:
        part_copy(q).start()

    at = lax.broadcasted_iota(jnp.int32, (ROWS, H), 0) + rel * ROWS
    bound = type_rows[0]
    row_bias = jnp.broadcast_to(bias[0:1, :], (ROWS, H))
    for c in range(1, 4):
        row_bias = jnp.where(at >= bound, bias[c : c + 1, :], row_bias)
        bound = bound + type_rows[c]
    for dx, dm in across + [(0, 1)]:
        fx, fm = (x - dx + NX) % NX, (mp + dm) % NM
        slot = fx * NM + fm
        remote(
            z_send.at[fm, fx], z_recv.at[slot], z_ss.at[slot], z_rs.at[slot],
            rel=fx * NC + core, mp=fm).wait_recv()
    total = z_recv[0].astype(F32)
    for q in range(1, NX * NM):
        total = total + z_recv[q].astype(F32)
    out[...] = (total + row_bias).astype(BF)

    for q in range(NQ):
        s_copy(q).wait_send()
    for dm in (1, 0):
        sib_copy((mp + dm) % NM).wait_send()
    for dx, dm in across + [(0, 1)]:
        z_copy(dx, dm).wait_send()
    for q in group:
        fd, fm = (dst - q // NM + ND) % ND, (mp + q % NM) % NM
        remote(p_send, p_recv.at[fd * NM + fm], p_ss.at[q], p_rs.at[q], dst=fd, mp=fm).wait_recv()
    total = p_recv[0]
    for q in range(1, ND * NM):
        total = total + p_recv[q]
    grad[...] = total
    for q in group:
        part_copy(q).wait_send()


def on_device(
    node_table, edge_weights, src_ids, dst_ids, block_mask,
    basis_coef, basis_mats, type_bias, type_rows, cotangent,
):
    anywhere = pl.BlockSpec(memory_space=pl.ANY)
    vmem = pl.BlockSpec(memory_space=pltpu.VMEM)
    dma = pltpu.SemaphoreType.DMA
    return pl.pallas_call(
        kernel,
        out_shape=(
            jax.ShapeDtypeStruct((ROWS, H), BF),
            jax.ShapeDtypeStruct((1, BASES), F32),
        ),
        in_specs=[anywhere] * 10,
        out_specs=(vmem, vmem),
        scratch_shapes=[
            pltpu.SMEM((1, 2 * ND), jnp.int32),
            pltpu.SMEM((1, BASES), F32),
            pltpu.SMEM((4,), jnp.int32),
            pltpu.VMEM((4, H), F32),
            pltpu.VMEM((TAB, H), BF),
            pltpu.VMEM((2 * ND, BLK, BLK), BF),
            pltpu.VMEM((2 * ND, BLK), jnp.int32),
            pltpu.VMEM((BASES, F, H), BF),
            pltpu.VMEM((CHUNK, TAB), BF),
            pltpu.VMEM((NQ, ND, CHUNK, Q), BF),
            pltpu.VMEM((NQ, ND, CHUNK, Q), BF),
            pltpu.VMEM((ND, 2, BLK), jnp.int32),
            pltpu.VMEM((OWN, CHUNK), BF),
            pltpu.VMEM((NQ, OWN, Q), F32),
            pltpu.VMEM((OWN, H), BF),
            pltpu.VMEM((NQ, Q, OWN), BF),
            pltpu.VMEM((NC, NM, NX, ROWS, H), BF),
            pltpu.VMEM((F, H), BF),
            pltpu.VMEM((NM, H, H), BF),
            pltpu.VMEM((NQ, Q, H), BF),
            pltpu.VMEM((NQ, Q, H), BF),
            pltpu.VMEM((F, H), F32),
            pltpu.VMEM((BASES, 8, 128), F32),
            pltpu.VMEM((NM, NX * ROWS, H), BF),
            pltpu.VMEM((NM, NX * ROWS, H), BF),
            pltpu.VMEM((NM, NX * ROWS, H), F32),
            pltpu.VMEM((NM, NX, ROWS, H), BF),
            pltpu.VMEM((NX * NM, ROWS, H), BF),
            pltpu.VMEM((BASES, 128), F32),
            pltpu.VMEM((1, BASES), F32),
            pltpu.VMEM((ND * NM, 1, BASES), F32),
            dma((10,)),
            dma((NQ, ND)), dma((NQ, ND)), dma((ND,)), dma((ND,)),
            dma((NX + 1,)), dma((NX + 1,)),
            dma((2,)), dma((NQ,)), dma((NQ,)), dma((NM,)), dma((NM,)),
            dma((NX * NM,)), dma((NX * NM,)),
            dma((ND * NM,)), dma((ND * NM,)),
        ],
        compiler_params=pltpu.CompilerParams(
            collective_id=0, has_side_effects=True, vmem_limit_bytes=67000000
        ),
        name="relational_layer",
    )(
        node_table, edge_weights[0], src_ids[0], dst_ids[0].reshape(ND, 2, BLK), block_mask,
        basis_coef, basis_mats, type_bias, type_rows, cotangent,
    )


def solution(mesh):
    in_specs = (
        P(("rel", "dst"), None),
        P("rel", "dst", None, None),
        P("rel", "dst", None),
        P("rel", "dst", None),
        P("rel", "dst"),
        P("rel", None),
        P(None, None, "mp"),
        P(None, "mp"),
        P(),
        P(("rel", "dst"), "mp"),
    )
    out_specs = (P(("rel", "dst"), "mp"), P("rel", None))
    return jax.shard_map(
        on_device, mesh=mesh, in_specs=in_specs, out_specs=out_specs, check_vma=False
    )
```

```python
import jax
import jax.numpy as jnp
from jax import lax
from jax.experimental import pallas as pl
from jax.experimental.pallas import tpu as pltpu
from jax.sharding import PartitionSpec as P

MESH = pl.DeviceIdType.MESH
BF = jnp.bfloat16
F32 = jnp.float32
NX, NC, NZ, NY, NM = 4, 2, 8, 2, 2
NR, ND = NX * NC, NZ * NY
TAB, F, H, BLK, ROWS, BASES = 1024, 512, 256, 128, 128, 32
OWN = NR * ROWS
CHUNK = 2 * BLK
NQ, Q = 2, 128
EARLY = 3


def offset(k):
    step = k // 2
    far = (step // 2 + 1) * (1 - 2 * (step % 2)) * (1 - step // (NZ - 1))
    return far, k % 2


def kernel(
    table, edge, src_ids, dst_ids, mask_any, coef_any, basis, bias_any, rows_any, cot,
    out, grad,
    mask, coef, type_rows, bias,
    tbl, edg, sid, bas, hot, sbuf, rbuf, ids, hot_t, acc, accb, acct, gbuf, wall, wbuf,
    s_send, s_recv, s_all, grad_sums, z_sib, z_sibr, z_own, z_send, z_recv, part, p_send, p_recv,
    load_sem, c_ss, c_rs, i_ss, i_rs, g_ss, g_rs, w_sem, s_ss, s_rs, sib_ss, sib_rs, z_ss, z_rs, p_ss, p_rs, word,
):
    rel, dst, mp = lax.axis_index("rel"), lax.axis_index("dst"), lax.axis_index("mp")
    x, core = rel // NC, rel % NC
    z, y = dst // NY, dst % NY
    other = 1 - mp

    def load(i, src, to):
        return pltpu.make_async_copy(src, to, load_sem.at[i])

    def remote(src, to, ss, rs, **where):
        return pltpu.make_async_remote_copy(src, to, ss, rs, device_id=where, device_id_type=MESH)

    barrier = pltpu.get_barrier_semaphore()
    group = sorted(range(1, ND * NM), key=lambda q: abs(q - ND))
    across = [(dx, dm) for dx in range(1, NX) for dm in range(NM)]

    def greet(**where):
        pl.semaphore_signal(barrier, inc=1, device_id=where, device_id_type=MESH)

    for q in group:
        greet(dst=(dst + q // NM) % ND, mp=(mp + q % NM) % NM)
    near_x = (1, NX - 1)
    for dx in near_x:
        greet(rel=(x + dx) % NX * NC + core)
    sibling = x * NC + 1 - core
    greet(rel=sibling)

    loads = [
        load(0, src_ids, sid),
        load(1, mask_any, mask),
        load(2, table.at[:, pl.ds(pl.multiple_of(mp * H, H), H)], tbl),
        load(3, edge, edg),
        load(4, dst_ids.at[dst], ids.at[dst]),
        load(5, cot, gbuf.at[core, mp, x]),
        load(6, coef_any, coef),
        load(7, rows_any, type_rows),
        load(8, bias_any, bias),
        load(9, basis, bas),
    ]
    for copy in loads[:9]:
        copy.start()

    lanes = lax.broadcasted_iota(jnp.int32, (BLK, BLK), 1)

    def make_chunk(d, to, at):
        for half in range(2):
            k = 2 * d + half
            row = sid[pl.ds(k, 1), :]
            col = jnp.broadcast_to(row, (BLK, BLK)).T
            for t in range(TAB // BLK):
                hot[half * BLK : (half + 1) * BLK, t * BLK : (t + 1) * BLK] = jnp.where(
                    lanes + t * BLK == col, 1.0, 0.0
                ).astype(BF)
        picked = jnp.dot(hot[...], tbl[...], preferred_element_type=F32).astype(BF)
        for half in range(2):
            k = 2 * d + half
            live = mask[0, k].astype(F32)
            block = (edg[k].astype(F32) * live).astype(BF)
            made = jnp.dot(
                block, picked[half * BLK : (half + 1) * BLK, :], preferred_element_type=F32
            ).astype(BF)
            for q in range(NQ):
                to[q, at, half * BLK : (half + 1) * BLK, :] = made[:, q * Q : (q + 1) * Q]

    def peer(k, sign):
        dz, dy = offset(k)
        return ((z + sign * dz + NZ) % NZ) * NY + (y + dy) % NY

    def kth(i):
        return i + i // (ND - 2)

    def id_copy(to):
        return remote(dst_ids.at[to], ids.at[dst], i_ss.at[to], i_rs.at[dst], dst=to)

    def chunk_copy(to, q):
        return remote(sbuf.at[q, to], rbuf.at[q, dst], c_ss.at[q, to], c_rs.at[q, dst], dst=to)

    def make(i, _):
        to = peer(kth(i), 1)
        make_chunk(to, sbuf, to)
        return 0

    def send(q):
        def start(i, _):
            chunk_copy(peer(kth(i), 1), q).start()
            return 0
        return start

    def send_ids(i, _):
        id_copy(peer(kth(i), 1)).start()
        return 0

    def make_send(i, _):
        make(i, 0)
        return send(0)(i, 0)

    for i in range(4):
        loads[i].wait()
    lax.fori_loop(0, EARLY, make, 0)
    loads[4].wait()
    loads[5].wait()
    pl.semaphore_wait(barrier, len(group) + len(near_x) + 1)

    def tell(level):
        for dx in near_x:
            pl.semaphore_signal(
                word.at[level], inc=1, device_id={"rel": (x + dx) % NX * NC + core}, device_id_type=MESH)

    tell(0)
    lax.fori_loop(0, EARLY, send(0), 0)
    lax.fori_loop(0, ND - 1, send_ids, 0)
    mine = gbuf.at[core, mp, x]
    g_pair = remote(mine, mine, g_ss.at[0], g_rs.at[0], mp=other)
    g_pair.start()
    loads[9].start()
    lax.fori_loop(EARLY, ND - 1, make_send, 0)
    lax.fori_loop(0, ND - 1, send(1), 0)
    make_chunk(dst, rbuf, dst)

    g_pair.wait_recv()

    def g_across(dx):
        both = gbuf.at[core, :, x]
        return remote(both, both, g_ss.at[dx], g_rs.at[dx], rel=(x + dx) % NX * NC + core)

    pl.semaphore_wait(word.at[0], len(near_x))
    tell(1)
    for dx in range(1, NX):
        g_across(dx).start()
    pl.semaphore_wait(word.at[1], len(near_x))

    for i in (6, 7, 8, 9):
        loads[i].wait()
    TILE = 32

    def mix(t, _):
        at = pl.multiple_of(t * TILE, TILE)
        total = coef[0, 0] * bas[0, pl.ds(at, TILE), :].astype(F32)
        for b in range(1, BASES):
            total = total + coef[0, b] * bas[b, pl.ds(at, TILE), :].astype(F32)
        wall[pl.ds(at, TILE), :] = total.astype(BF)
        return 0

    lax.fori_loop(0, F // TILE, mix, 0)
    w_copy = remote(wall.at[pl.ds(pl.multiple_of(other * H, H), H)], wbuf.at[mp], w_sem.at[0], w_sem.at[1], mp=other)
    w_copy.start()
    wbuf[mp] = wall[pl.ds(pl.multiple_of(mp * H, H), H), :]

    place = lax.broadcasted_iota(jnp.int32, (OWN, BLK), 0)
    half_rows = NX * ROWS
    rows = ((place % half_rows) // ROWS * NC + place // half_rows) * ROWS + place % ROWS

    def add_chunk(s, q):
        for half in range(2):
            row = ids[s, half : half + 1, :]
            hot_t[:, half * BLK : (half + 1) * BLK] = jnp.where(rows == row, 1.0, 0.0).astype(BF)
        return jnp.dot(hot_t[...], rbuf[q, s], preferred_element_type=F32)

    for q in range(NQ):
        acc[q] = add_chunk(dst, q)

    def take(i, q):
        s = peer(kth(i), -1)
        if q == 0:
            remote(dst_ids.at[s], ids.at[s], i_ss.at[s], i_rs.at[s], dst=s).wait_recv()
        remote(sbuf.at[q, s], rbuf.at[q, s], c_ss.at[q, s], c_rs.at[q, s], dst=s).wait_recv()
        return add_chunk(s, q)

    def take_chunk(q):
        def step(i, _):
            acc[q] += take(i, q)
            return 0
        return step

    def outer(g, q):
        return jnp.dot(acct[q], gbuf[:, g].reshape(OWN, H), preferred_element_type=F32)

    def s_copy(q):
        return remote(s_send.at[q], s_recv.at[q], s_ss.at[q], s_rs.at[q], mp=other)

    def s_rows(m, q):
        return pl.multiple_of(m * H + q * Q, Q)

    def sums_final(q, total):
        half = total.astype(BF)
        accb[:, q * Q : (q + 1) * Q] = half
        acct[q] = half.T
        s_send[q] = outer(other, q).astype(BF)
        s_copy(q).start()

    DT = 16

    def against(m, q):
        base = s_rows(m, q)
        def step(t, sums):
            at = pl.multiple_of(base + t * DT, DT)
            s = s_all[pl.ds(at, DT), :]
            new = []
            for b in range(BASES):
                v = bas[b, pl.ds(at, DT), :].astype(F32) * s
                v = (v[0:8, 0:128] + v[8:16, 0:128]) + (v[0:8, 128:256] + v[8:16, 128:256])
                new.append(sums[b] + v)
            return tuple(new)
        first = tuple(grad_sums[b] for b in range(BASES))
        sums = lax.fori_loop(0, Q // DT, step, first)
        for b in range(BASES):
            grad_sums[b] = sums[b]

    def against_own(q):
        s_all[pl.ds(s_rows(mp, q), Q), :] = outer(mp, q)
        against(mp, q)

    def against_other(q):
        s_copy(q).wait_recv()
        s_all[pl.ds(s_rows(other, q), Q), :] = s_recv[q].astype(F32)
        against(other, q)

    grad_sums[...] = jnp.zeros_like(grad_sums)
    lax.fori_loop(0, 4, take_chunk(0), 0)

    for dx in range(1, NX):
        theirs = gbuf.at[core, :, (x - dx + NX) % NX]
        remote(theirs, theirs, g_ss.at[dx], g_rs.at[dx], rel=(x - dx + NX) % NX * NC + core).wait_recv()
    g_sib = remote(gbuf.at[core], gbuf.at[core], g_ss.at[NX], g_rs.at[NX], rel=sibling)
    g_sib.start()

    lax.fori_loop(4, ND - 1, take_chunk(0), 0)
    g_sib.wait_recv()
    sums_final(0, acc[0])
    lax.fori_loop(0, 2, take_chunk(1), 0)
    against_own(0)
    lax.fori_loop(2, 6, take_chunk(1), 0)
    against_other(0)
    w_copy.wait_recv()
    lax.fori_loop(6, ND - 2, take_chunk(1), 0)
    sums_final(1, acc[1] + take(ND - 2, 1))

    def times_w(c, g):
        return jnp.dot(
            accb[pl.ds(pl.multiple_of(c * half_rows, half_rows), half_rows), :], wbuf[g],
            preferred_element_type=F32)

    def sib_copy(g):
        return remote(z_sib.at[g], z_sibr.at[g], sib_ss.at[g], sib_rs.at[g], rel=sibling)

    columns = (other, mp)
    for g in columns:
        z_sib[g] = times_w(1 - core, g).astype(BF)
        sib_copy(g).start()
    for g in columns:
        z_own[g] = times_w(core, g)

    def z_copy(dx, dm):
        tx, tm = (x + dx) % NX, (mp + dm) % NM
        return remote(
            z_send.at[tm, tx], z_recv.at[x * NM + mp], z_ss.at[tx * NM + tm], z_rs.at[x * NM + mp],
            rel=tx * NC + core, mp=tm)

    order = (2, 1, 3, 0)
    for dm in (1, 0):
        g = (mp + dm) % NM
        sib_copy(g).wait_recv()
        for dx in order:
            tx = (x + dx) % NX
            at = pl.ds(pl.multiple_of(tx * ROWS, ROWS), ROWS)
            piece = (z_own[g, at, :] + z_sibr[g, at, :].astype(F32)).astype(BF)
            if dx or dm:
                z_send[g, tx] = piece
                z_copy(dx, dm).start()
            else:
                z_recv[x * NM + mp] = piece

    against_own(1)

    def done_chunk(i, _):
        to = peer(kth(i), 1)
        id_copy(to).wait_send()
        for q in range(NQ):
            chunk_copy(to, q).wait_send()
        return 0

    lax.fori_loop(0, ND - 1, done_chunk, 0)
    g_pair.wait_send()
    for dx in range(1, NX):
        g_across(dx).wait_send()
    g_sib.wait_send()
    w_copy.wait_send()

    against_other(1)
    for b in range(BASES):
        part[b : b + 1, :] = jnp.sum(grad_sums[b], axis=0, keepdims=True)
    total = jnp.sum(part[...].T, axis=0, keepdims=True)
    me = dst * NM + mp
    p_send[...] = total
    p_recv[me] = total

    def part_copy(q):
        td, tm = (dst + q // NM) % ND, (mp + q % NM) % NM
        return remote(p_send, p_recv.at[me], p_ss.at[q], p_rs.at[q], dst=td, mp=tm)

    for q in group:
        part_copy(q).start()

    at = lax.broadcasted_iota(jnp.int32, (ROWS, H), 0) + rel * ROWS
    bound = type_rows[0]
    row_bias = jnp.broadcast_to(bias[0:1, :], (ROWS, H))
    for c in range(1, 4):
        row_bias = jnp.where(at >= bound, bias[c : c + 1, :], row_bias)
        bound = bound + type_rows[c]
    for dx, dm in across + [(0, 1)]:
        fx, fm = (x - dx + NX) % NX, (mp + dm) % NM
        slot = fx * NM + fm
        remote(
            z_send.at[fm, fx], z_recv.at[slot], z_ss.at[slot], z_rs.at[slot],
            rel=fx * NC + core, mp=fm).wait_recv()
    total = z_recv[0].astype(F32)
    for q in range(1, NX * NM):
        total = total + z_recv[q].astype(F32)
    out[...] = (total + row_bias).astype(BF)

    for q in range(NQ):
        s_copy(q).wait_send()
    for dm in (1, 0):
        sib_copy((mp + dm) % NM).wait_send()
    for dx, dm in across + [(0, 1)]:
        z_copy(dx, dm).wait_send()
    for q in group:
        fd, fm = (dst - q // NM + ND) % ND, (mp + q % NM) % NM
        remote(p_send, p_recv.at[fd * NM + fm], p_ss.at[q], p_rs.at[q], dst=fd, mp=fm).wait_recv()
    total = p_recv[0]
    for q in range(1, ND * NM):
        total = total + p_recv[q]
    grad[...] = total
    for q in group:
        part_copy(q).wait_send()


def on_device(
    node_table, edge_weights, src_ids, dst_ids, block_mask,
    basis_coef, basis_mats, type_bias, type_rows, cotangent,
):
    anywhere = pl.BlockSpec(memory_space=pl.ANY)
    vmem = pl.BlockSpec(memory_space=pltpu.VMEM)
    dma = pltpu.SemaphoreType.DMA
    return pl.pallas_call(
        kernel,
        out_shape=(
            jax.ShapeDtypeStruct((ROWS, H), BF),
            jax.ShapeDtypeStruct((1, BASES), F32),
        ),
        in_specs=[anywhere] * 10,
        out_specs=(vmem, vmem),
        scratch_shapes=[
            pltpu.SMEM((1, 2 * ND), jnp.int32),
            pltpu.SMEM((1, BASES), F32),
            pltpu.SMEM((4,), jnp.int32),
            pltpu.VMEM((4, H), F32),
            pltpu.VMEM((TAB, H), BF),
            pltpu.VMEM((2 * ND, BLK, BLK), BF),
            pltpu.VMEM((2 * ND, BLK), jnp.int32),
            pltpu.VMEM((BASES, F, H), BF),
            pltpu.VMEM((CHUNK, TAB), BF),
            pltpu.VMEM((NQ, ND, CHUNK, Q), BF),
            pltpu.VMEM((NQ, ND, CHUNK, Q), BF),
            pltpu.VMEM((ND, 2, BLK), jnp.int32),
            pltpu.VMEM((OWN, CHUNK), BF),
            pltpu.VMEM((NQ, OWN, Q), F32),
            pltpu.VMEM((OWN, H), BF),
            pltpu.VMEM((NQ, Q, OWN), BF),
            pltpu.VMEM((NC, NM, NX, ROWS, H), BF),
            pltpu.VMEM((F, H), BF),
            pltpu.VMEM((NM, H, H), BF),
            pltpu.VMEM((NQ, Q, H), BF),
            pltpu.VMEM((NQ, Q, H), BF),
            pltpu.VMEM((F, H), F32),
            pltpu.VMEM((BASES, 8, 128), F32),
            pltpu.VMEM((NM, NX * ROWS, H), BF),
            pltpu.VMEM((NM, NX * ROWS, H), BF),
            pltpu.VMEM((NM, NX * ROWS, H), F32),
            pltpu.VMEM((NM, NX, ROWS, H), BF),
            pltpu.VMEM((NX * NM, ROWS, H), BF),
            pltpu.VMEM((BASES, 128), F32),
            pltpu.VMEM((1, BASES), F32),
            pltpu.VMEM((ND * NM, 1, BASES), F32),
            dma((10,)),
            dma((NQ, ND)), dma((NQ, ND)), dma((ND,)), dma((ND,)),
            dma((NX + 1,)), dma((NX + 1,)),
            dma((2,)), dma((NQ,)), dma((NQ,)), dma((NM,)), dma((NM,)),
            dma((NX * NM,)), dma((NX * NM,)),
            dma((ND * NM,)), dma((ND * NM,)),
            pltpu.SemaphoreType.REGULAR((2,)),
        ],
        compiler_params=pltpu.CompilerParams(
            collective_id=0, has_side_effects=True, vmem_limit_bytes=67000000
        ),
        name="relational_layer",
    )(
        node_table, edge_weights[0], src_ids[0], dst_ids[0].reshape(ND, 2, BLK), block_mask,
        basis_coef, basis_mats, type_bias, type_rows, cotangent,
    )


def solution(mesh):
    in_specs = (
        P(("rel", "dst"), None),
        P("rel", "dst", None, None),
        P("rel", "dst", None),
        P("rel", "dst", None),
        P("rel", "dst"),
        P("rel", None),
        P(None, None, "mp"),
        P(None, "mp"),
        P(),
        P(("rel", "dst"), "mp"),
    )
    out_specs = (P(("rel", "dst"), "mp"), P("rel", None))
    return jax.shard_map(
        on_device, mesh=mesh, in_specs=in_specs, out_specs=out_specs, check_vma=False
    )
```

```python
import jax
import jax.numpy as jnp
from jax import lax
from jax.experimental import pallas as pl
from jax.experimental.pallas import tpu as pltpu
from jax.sharding import PartitionSpec as P

MESH = pl.DeviceIdType.MESH
BF = jnp.bfloat16
F32 = jnp.float32
NX, NC, NZ, NY, NM = 4, 2, 8, 2, 2
NR, ND = NX * NC, NZ * NY
TAB, F, H, BLK, ROWS, BASES = 1024, 512, 256, 128, 128, 32
OWN = NR * ROWS
CHUNK = 2 * BLK
NQ, Q = 2, 128
EARLY = 3


def offset(k):
    step = k // 2
    far = (step // 2 + 1) * (1 - 2 * (step % 2)) * (1 - step // (NZ - 1))
    return far, k % 2


def kernel(
    table, edge, src_ids, dst_ids, mask_any, coef_any, basis, bias_any, rows_any, cot,
    out, grad,
    mask, coef, type_rows, bias,
    tbl, edg, sid, bas, hot, sbuf, rbuf, ids, hot_t, acc, accb, acct, gbuf, wall, wbuf,
    s_send, s_recv, s_all, grad_sums, z_sib, z_sibr, z_own, z_send, z_recv, part, p_send, p_recv,
    load_sem, c_ss, c_rs, i_ss, i_rs, g_ss, g_rs, w_sem, s_ss, s_rs, sib_ss, sib_rs, z_ss, z_rs, p_ss, p_rs, word,
):
    rel, dst, mp = lax.axis_index("rel"), lax.axis_index("dst"), lax.axis_index("mp")
    x, core = rel // NC, rel % NC
    z, y = dst // NY, dst % NY
    other = 1 - mp

    def load(i, src, to):
        return pltpu.make_async_copy(src, to, load_sem.at[i])

    def remote(src, to, ss, rs, **where):
        return pltpu.make_async_remote_copy(src, to, ss, rs, device_id=where, device_id_type=MESH)

    barrier = pltpu.get_barrier_semaphore()
    group = sorted(range(1, ND * NM), key=lambda q: abs(q - ND))
    across = [(dx, dm) for dx in range(1, NX) for dm in range(NM)]

    def greet(**where):
        pl.semaphore_signal(barrier, inc=1, device_id=where, device_id_type=MESH)

    for q in group:
        greet(dst=(dst + q // NM) % ND, mp=(mp + q % NM) % NM)
    near_x = (1, NX - 1)
    for dx in near_x:
        greet(rel=(x + dx) % NX * NC + core)
    sibling = x * NC + 1 - core
    greet(rel=sibling)

    loads = [
        load(0, src_ids, sid),
        load(1, mask_any, mask),
        load(2, table.at[:, pl.ds(pl.multiple_of(mp * H, H), H)], tbl),
        load(3, edge, edg),
        load(4, dst_ids.at[dst], ids.at[dst]),
        load(5, cot, gbuf.at[core, mp, x]),
        load(6, coef_any, coef),
        load(7, rows_any, type_rows),
        load(8, bias_any, bias),
        load(9, basis, bas),
    ]
    for copy in loads[:9]:
        copy.start()

    lanes = lax.broadcasted_iota(jnp.int32, (BLK, BLK), 1)

    def make_chunk(d, to, at):
        for half in range(2):
            k = 2 * d + half
            row = sid[pl.ds(k, 1), :]
            col = jnp.broadcast_to(row, (BLK, BLK)).T
            for t in range(TAB // BLK):
                hot[half * BLK : (half + 1) * BLK, t * BLK : (t + 1) * BLK] = jnp.where(
                    lanes + t * BLK == col, 1.0, 0.0
                ).astype(BF)
        picked = jnp.dot(hot[...], tbl[...], preferred_element_type=F32).astype(BF)
        for half in range(2):
            k = 2 * d + half
            live = mask[0, k].astype(F32)
            block = (edg[k].astype(F32) * live).astype(BF)
            made = jnp.dot(
                block, picked[half * BLK : (half + 1) * BLK, :], preferred_element_type=F32
            ).astype(BF)
            for q in range(NQ):
                to[q, at, half * BLK : (half + 1) * BLK, :] = made[:, q * Q : (q + 1) * Q]

    def peer(k, sign):
        dz, dy = offset(k)
        return ((z + sign * dz + NZ) % NZ) * NY + (y + dy) % NY

    def kth(i):
        return i + i // (ND - 2)

    def id_copy(to):
        return remote(dst_ids.at[to], ids.at[dst], i_ss.at[to], i_rs.at[dst], dst=to)

    def chunk_copy(to, q):
        return remote(sbuf.at[q, to], rbuf.at[q, dst], c_ss.at[q, to], c_rs.at[q, dst], dst=to)

    def make(i, _):
        to = peer(kth(i), 1)
        make_chunk(to, sbuf, to)
        return 0

    def send(q):
        def start(i, _):
            chunk_copy(peer(kth(i), 1), q).start()
            return 0
        return start

    def send_ids(i, _):
        id_copy(peer(kth(i), 1)).start()
        return 0

    def make_send(i, _):
        make(i, 0)
        return send(0)(i, 0)

    for i in range(4):
        loads[i].wait()
    lax.fori_loop(0, EARLY, make, 0)
    loads[4].wait()
    loads[5].wait()
    pl.semaphore_wait(barrier, len(group) + len(near_x) + 1)

    def tell(level):
        for dx in near_x:
            pl.semaphore_signal(
                word.at[level], inc=1, device_id={"rel": (x + dx) % NX * NC + core}, device_id_type=MESH)

    tell(0)
    lax.fori_loop(0, EARLY, send(0), 0)
    lax.fori_loop(0, ND - 1, send_ids, 0)
    mine = gbuf.at[core, mp, x]
    g_pair = remote(mine, mine, g_ss.at[0], g_rs.at[0], mp=other)
    g_pair.start()
    loads[9].start()
    lax.fori_loop(EARLY, ND - 1, make_send, 0)
    lax.fori_loop(0, ND - 1, send(1), 0)
    make_chunk(dst, rbuf, dst)

    g_pair.wait_recv()

    def g_across(dx):
        both = gbuf.at[core, :, x]
        return remote(both, both, g_ss.at[dx], g_rs.at[dx], rel=(x + dx) % NX * NC + core)

    pl.semaphore_wait(word.at[0], len(near_x))
    tell(1)
    for dx in range(1, NX):
        g_across(dx).start()
    pl.semaphore_wait(word.at[1], len(near_x))

    for i in (6, 7, 8, 9):
        loads[i].wait()
    TILE = 32

    def mix(t, _):
        at = pl.multiple_of(t * TILE, TILE)
        total = coef[0, 0] * bas[0, pl.ds(at, TILE), :].astype(F32)
        for b in range(1, BASES):
            total = total + coef[0, b] * bas[b, pl.ds(at, TILE), :].astype(F32)
        wall[pl.ds(at, TILE), :] = total.astype(BF)
        return 0

    lax.fori_loop(0, F // TILE, mix, 0)
    w_copy = remote(wall.at[pl.ds(pl.multiple_of(other * H, H), H)], wbuf.at[mp], w_sem.at[0], w_sem.at[1], mp=other)
    w_copy.start()
    wbuf[mp] = wall[pl.ds(pl.multiple_of(mp * H, H), H), :]

    place = lax.broadcasted_iota(jnp.int32, (OWN, BLK), 0)
    half_rows = NX * ROWS
    rows = ((place % half_rows) // ROWS * NC + place // half_rows) * ROWS + place % ROWS

    def add_chunk(s, q):
        for half in range(2):
            row = ids[s, half : half + 1, :]
            hot_t[:, half * BLK : (half + 1) * BLK] = jnp.where(rows == row, 1.0, 0.0).astype(BF)
        return jnp.dot(hot_t[...], rbuf[q, s], preferred_element_type=F32)

    for q in range(NQ):
        acc[q] = add_chunk(dst, q)

    def take(i, q):
        s = peer(kth(i), -1)
        if q == 0:
            remote(dst_ids.at[s], ids.at[s], i_ss.at[s], i_rs.at[s], dst=s).wait_recv()
        remote(sbuf.at[q, s], rbuf.at[q, s], c_ss.at[q, s], c_rs.at[q, s], dst=s).wait_recv()
        return add_chunk(s, q)

    def take_chunk(q):
        def step(i, _):
            acc[q] += take(i, q)
            return 0
        return step

    def outer(g, q):
        return jnp.dot(acct[q], gbuf[:, g].reshape(OWN, H), preferred_element_type=F32)

    def s_copy(q):
        return remote(s_send.at[q], s_recv.at[q], s_ss.at[q], s_rs.at[q], mp=other)

    def s_rows(m, q):
        return pl.multiple_of(m * H + q * Q, Q)

    def sums_final(q, total):
        half = total.astype(BF)
        accb[:, q * Q : (q + 1) * Q] = half
        acct[q] = half.T
        s_send[q] = outer(other, q).astype(BF)
        s_copy(q).start()

    DT = 16

    def against(m, q):
        base = s_rows(m, q)
        def step(t, sums):
            at = pl.multiple_of(base + t * DT, DT)
            s = s_all[pl.ds(at, DT), :]
            new = []
            for b in range(BASES):
                v = bas[b, pl.ds(at, DT), :].astype(F32) * s
                v = (v[0:8, 0:128] + v[8:16, 0:128]) + (v[0:8, 128:256] + v[8:16, 128:256])
                new.append(sums[b] + v)
            return tuple(new)
        first = tuple(grad_sums[b] for b in range(BASES))
        sums = lax.fori_loop(0, Q // DT, step, first)
        for b in range(BASES):
            grad_sums[b] = sums[b]

    def against_own(q):
        s_all[pl.ds(s_rows(mp, q), Q), :] = outer(mp, q)
        against(mp, q)

    def against_other(q):
        s_copy(q).wait_recv()
        s_all[pl.ds(s_rows(other, q), Q), :] = s_recv[q].astype(F32)
        against(other, q)

    grad_sums[...] = jnp.zeros_like(grad_sums)
    lax.fori_loop(0, 4, take_chunk(0), 0)

    for dx in range(1, NX):
        theirs = gbuf.at[core, :, (x - dx + NX) % NX]
        remote(theirs, theirs, g_ss.at[dx], g_rs.at[dx], rel=(x - dx + NX) % NX * NC + core).wait_recv()
    g_sib = remote(gbuf.at[core], gbuf.at[core], g_ss.at[NX], g_rs.at[NX], rel=sibling)
    g_sib.start()

    lax.fori_loop(4, ND - 1, take_chunk(0), 0)
    g_sib.wait_recv()
    sums_final(0, acc[0])
    lax.fori_loop(0, 2, take_chunk(1), 0)
    against_own(0)
    lax.fori_loop(2, 6, take_chunk(1), 0)
    against_other(0)
    w_copy.wait_recv()
    lax.fori_loop(6, ND - 2, take_chunk(1), 0)
    sums_final(1, acc[1] + take(ND - 2, 1))

    def times_w(c, g):
        return jnp.dot(
            accb[pl.ds(pl.multiple_of(c * half_rows, half_rows), half_rows), :], wbuf[g],
            preferred_element_type=F32)

    def z_rows(tx):
        return pl.ds(pl.multiple_of(tx * ROWS, ROWS), ROWS)

    def sib_copy(g, tx):
        return remote(
            z_sib.at[g, z_rows(tx)], z_sibr.at[g, z_rows(tx)], sib_ss.at[g, tx], sib_rs.at[g, tx], rel=sibling)

    columns = (other, mp)
    order = (2, 1, 3, 0)
    for g in columns:
        for dx in order:
            tx = (x + dx) % NX
            first = pl.multiple_of((1 - core) * half_rows + tx * ROWS, ROWS)
            z_sib[g, z_rows(tx), :] = jnp.dot(
                accb[pl.ds(first, ROWS), :], wbuf[g], preferred_element_type=F32).astype(BF)
            sib_copy(g, tx).start()
    for g in columns:
        z_own[g] = times_w(core, g)

    def z_copy(dx, dm):
        tx, tm = (x + dx) % NX, (mp + dm) % NM
        return remote(
            z_send.at[tm, tx], z_recv.at[x * NM + mp], z_ss.at[tx * NM + tm], z_rs.at[x * NM + mp],
            rel=tx * NC + core, mp=tm)

    for dm in (1, 0):
        g = (mp + dm) % NM
        for dx in order:
            tx = (x + dx) % NX
            at = z_rows(tx)
            sib_copy(g, tx).wait_recv()
            piece = (z_own[g, at, :] + z_sibr[g, at, :].astype(F32)).astype(BF)
            if dx or dm:
                z_send[g, tx] = piece
                z_copy(dx, dm).start()
            else:
                z_recv[x * NM + mp] = piece

    against_own(1)

    def done_chunk(i, _):
        to = peer(kth(i), 1)
        id_copy(to).wait_send()
        for q in range(NQ):
            chunk_copy(to, q).wait_send()
        return 0

    lax.fori_loop(0, ND - 1, done_chunk, 0)
    g_pair.wait_send()
    for dx in range(1, NX):
        g_across(dx).wait_send()
    g_sib.wait_send()
    w_copy.wait_send()

    against_other(1)
    for b in range(BASES):
        part[b : b + 1, :] = jnp.sum(grad_sums[b], axis=0, keepdims=True)
    total = jnp.sum(part[...].T, axis=0, keepdims=True)
    me = dst * NM + mp
    p_send[...] = total
    p_recv[me] = total

    def part_copy(q):
        td, tm = (dst + q // NM) % ND, (mp + q % NM) % NM
        return remote(p_send, p_recv.at[me], p_ss.at[q], p_rs.at[q], dst=td, mp=tm)

    for q in group:
        part_copy(q).start()

    at = lax.broadcasted_iota(jnp.int32, (ROWS, H), 0) + rel * ROWS
    bound = type_rows[0]
    row_bias = jnp.broadcast_to(bias[0:1, :], (ROWS, H))
    for c in range(1, 4):
        row_bias = jnp.where(at >= bound, bias[c : c + 1, :], row_bias)
        bound = bound + type_rows[c]
    total = row_bias + z_recv[x * NM + mp].astype(F32)
    for dx, dm in across + [(0, 1)]:
        fx, fm = (x - dx + NX) % NX, (mp + dm) % NM
        slot = fx * NM + fm
        remote(
            z_send.at[fm, fx], z_recv.at[slot], z_ss.at[slot], z_rs.at[slot],
            rel=fx * NC + core, mp=fm).wait_recv()
        total = total + z_recv[slot].astype(F32)
    out[...] = total.astype(BF)

    for q in range(NQ):
        s_copy(q).wait_send()
    for dm in (1, 0):
        for tx in range(NX):
            sib_copy((mp + dm) % NM, tx).wait_send()
    for dx, dm in across + [(0, 1)]:
        z_copy(dx, dm).wait_send()
    for q in group:
        fd, fm = (dst - q // NM + ND) % ND, (mp + q % NM) % NM
        remote(p_send, p_recv.at[fd * NM + fm], p_ss.at[q], p_rs.at[q], dst=fd, mp=fm).wait_recv()
    total = p_recv[0]
    for q in range(1, ND * NM):
        total = total + p_recv[q]
    grad[...] = total
    for q in group:
        part_copy(q).wait_send()


def on_device(
    node_table, edge_weights, src_ids, dst_ids, block_mask,
    basis_coef, basis_mats, type_bias, type_rows, cotangent,
):
    anywhere = pl.BlockSpec(memory_space=pl.ANY)
    vmem = pl.BlockSpec(memory_space=pltpu.VMEM)
    dma = pltpu.SemaphoreType.DMA
    return pl.pallas_call(
        kernel,
        out_shape=(
            jax.ShapeDtypeStruct((ROWS, H), BF),
            jax.ShapeDtypeStruct((1, BASES), F32),
        ),
        in_specs=[anywhere] * 10,
        out_specs=(vmem, vmem),
        scratch_shapes=[
            pltpu.SMEM((1, 2 * ND), jnp.int32),
            pltpu.SMEM((1, BASES), F32),
            pltpu.SMEM((4,), jnp.int32),
            pltpu.VMEM((4, H), F32),
            pltpu.VMEM((TAB, H), BF),
            pltpu.VMEM((2 * ND, BLK, BLK), BF),
            pltpu.VMEM((2 * ND, BLK), jnp.int32),
            pltpu.VMEM((BASES, F, H), BF),
            pltpu.VMEM((CHUNK, TAB), BF),
            pltpu.VMEM((NQ, ND, CHUNK, Q), BF),
            pltpu.VMEM((NQ, ND, CHUNK, Q), BF),
            pltpu.VMEM((ND, 2, BLK), jnp.int32),
            pltpu.VMEM((OWN, CHUNK), BF),
            pltpu.VMEM((NQ, OWN, Q), F32),
            pltpu.VMEM((OWN, H), BF),
            pltpu.VMEM((NQ, Q, OWN), BF),
            pltpu.VMEM((NC, NM, NX, ROWS, H), BF),
            pltpu.VMEM((F, H), BF),
            pltpu.VMEM((NM, H, H), BF),
            pltpu.VMEM((NQ, Q, H), BF),
            pltpu.VMEM((NQ, Q, H), BF),
            pltpu.VMEM((F, H), F32),
            pltpu.VMEM((BASES, 8, 128), F32),
            pltpu.VMEM((NM, NX * ROWS, H), BF),
            pltpu.VMEM((NM, NX * ROWS, H), BF),
            pltpu.VMEM((NM, NX * ROWS, H), F32),
            pltpu.VMEM((NM, NX, ROWS, H), BF),
            pltpu.VMEM((NX * NM, ROWS, H), BF),
            pltpu.VMEM((BASES, 128), F32),
            pltpu.VMEM((1, BASES), F32),
            pltpu.VMEM((ND * NM, 1, BASES), F32),
            dma((10,)),
            dma((NQ, ND)), dma((NQ, ND)), dma((ND,)), dma((ND,)),
            dma((NX + 1,)), dma((NX + 1,)),
            dma((2,)), dma((NQ,)), dma((NQ,)), dma((NM, NX)), dma((NM, NX)),
            dma((NX * NM,)), dma((NX * NM,)),
            dma((ND * NM,)), dma((ND * NM,)),
            pltpu.SemaphoreType.REGULAR((2,)),
        ],
        compiler_params=pltpu.CompilerParams(
            collective_id=0, has_side_effects=True, vmem_limit_bytes=67000000
        ),
        name="relational_layer",
    )(
        node_table, edge_weights[0], src_ids[0], dst_ids[0].reshape(ND, 2, BLK), block_mask,
        basis_coef, basis_mats, type_bias, type_rows, cotangent,
    )


def solution(mesh):
    in_specs = (
        P(("rel", "dst"), None),
        P("rel", "dst", None, None),
        P("rel", "dst", None),
        P("rel", "dst", None),
        P("rel", "dst"),
        P("rel", None),
        P(None, None, "mp"),
        P(None, "mp"),
        P(),
        P(("rel", "dst"), "mp"),
    )
    out_specs = (P(("rel", "dst"), "mp"), P("rel", None))
    return jax.shard_map(
        on_device, mesh=mesh, in_specs=in_specs, out_specs=out_specs, check_vma=False
    )
```
